32 devices in a mesh: chain: 4 (over x, core), blk: 8 (over z, y).
Axes of the slice: x: 2, y: 2, z: 4, core: 2. Of those that a mesh axis runs over, the one named last changes fastest.
Arguments:
- schur: bfloat16 [8192, 2048], P(('chain', 'blk')), as said below
- coupling: bfloat16 [8192, 2048], P(('chain', 'blk')), may hold values from -0.0625 to 0.0625
- next_diag: float32 [8192, 2048], P(('chain', 'blk')), as said below
Outputs:
- factor: float32 [8192, 2048], P(('chain', 'blk'))
- next_schur: float32 [8192, 2048], P(('chain', 'blk'))
The draws below stay inside these ranges and needn't reach their ends.
Inputs may be any that keep to these rules, and one draw needn't show every extreme that they name: `schur`: every slab's block is symmetric positive definite. `next_diag`: every slab's block is symmetric positive definite.
All inputs are finite; a program needn't handle non-finite values.
Results may differ from the reference program's by a relative error of at most 0.0034.
Values may be sent and summed in bfloat16 or wider, within the bound.
A program may use at most 128 MiB of HBM per device.

```python
import jax
import jax.numpy as jnp
from jax import lax

NB = 2048
SLABS = 4


def spd_slabs(key, floor_value):
    noise_key, shift_key = jax.random.split(key)
    raw = jax.random.normal(noise_key, (SLABS, NB, NB), jnp.float32)
    floor_part = floor_value * (1.0 + 0.5 * jax.random.uniform(shift_key, (SLABS, NB), jnp.float32))
    gram = jnp.einsum('sij,skj->sik', raw, raw, precision=lax.Precision.HIGHEST) / jnp.float32(NB)
    matrix = gram + floor_part[:, :, None] * jnp.eye(NB, dtype=jnp.float32)[None, :, :]
    return matrix.reshape(SLABS * NB, NB)


def draw_schur(key, part):
    return spd_slabs(jax.random.fold_in(key, 11), 0.02).astype(jnp.bfloat16)


def draw_next_diag(key, part):
    return spd_slabs(jax.random.fold_in(key, 23), 2.0)


def steps_of(own_key, shape, pieces, least, largest):
    level, own = 1.0, jax.random.fold_in(own_key, 6)
    for axis_at, parts in pieces:
        steps = jnp.exp(jax.random.uniform(jax.random.fold_in(own, axis_at), (parts,), jnp.float32, least / len(pieces), largest / len(pieces)))
        level = level * jnp.repeat(steps, shape[axis_at] // parts).reshape([-1 if axis == axis_at else 1 for axis in range(len(shape))])
    return level


def normal_values(key, dims, spread, most, shards=(), held_as=jnp.bfloat16):
    gain = steps_of(key, dims, shards, -0.22, 0.18) if shards else 1.0
    values = jax.random.normal(key, dims, jnp.float32) * spread * gain
    return jnp.minimum(jnp.maximum(values, -most), most).astype(held_as)


def setup_inputs(seed: int = 0) -> dict:
    keys = jax.random.split(jax.random.key(seed), 4)
    return {
        "schur": draw_schur(jax.random.fold_in(keys[3], 71), 0),
        "coupling": normal_values(keys[1], (SLABS * NB, NB), (4 * NB) ** -0.5, 0.0625, ((0, 32),)),
        "next_diag": draw_next_diag(jax.random.fold_in(keys[3], 71), 0),
    }


def factor_slab(blocks_pair):
    diag_block, couple_block = blocks_pair
    lower = jnp.linalg.cholesky(diag_block.astype(jnp.float32))
    solved = lax.linalg.triangular_solve(lower, couple_block.astype(jnp.float32).T, left_side=True, lower=True).astype(jnp.bfloat16)
    update = jnp.dot(solved.T.astype(jnp.float32), solved.astype(jnp.float32), preferred_element_type=jnp.float32)
    return (lower, update)

def reference(schur, coupling, next_diag):
    blocks = schur.reshape(SLABS, NB, NB)
    couple = coupling.reshape(SLABS, NB, NB)
    factors, updates = lax.map(factor_slab, (blocks, couple))
    shifted = jnp.concatenate([jnp.zeros((1, NB, NB), jnp.float32), updates[:-1]], axis=0)
    fresh = next_diag.reshape(SLABS, NB, NB) - shifted
    return (factors.reshape(SLABS * NB, NB), fresh.reshape(SLABS * NB, NB))
```

```python
import functools
import jax
import jax.numpy as jnp
from jax import lax
from jax.experimental import pallas as pl
from jax.experimental.pallas import tpu as pltpu
from jax.sharding import PartitionSpec as P

B = 128
T = 2 * B
BF = jnp.bfloat16
F32 = jnp.float32
MESH = pl.DeviceIdType.MESH


def split(x):
    hi = x.astype(BF)
    return hi, (x - hi.astype(F32)).astype(BF)


def dot_t(a, b):
    return lax.dot_general(a, b, (((1,), (1,)), ((), ())), preferred_element_type=F32)


def pair(x):
    return jnp.concatenate(split(x), 1)


def product_t(a, b):
    half = a.shape[1] // 2
    return dot_t(jnp.concatenate([a[:, :half], a], 1), jnp.concatenate([b, b[:, :half]], 1))


def product(a, b):
    ah, al = split(a)
    bh, bl = split(b)
    return jnp.dot(
        jnp.concatenate([ah, ah, al], 1), jnp.concatenate([bh, bl, bh], 0), preferred_element_type=F32
    )


def invert(block):
    size = block.shape[0]
    group = 8
    count = size // group
    sub = lax.broadcasted_iota(jnp.int32, (group, size), 0)
    lane = lax.broadcasted_iota(jnp.int32, (group, size), 1)
    rows = [block[group * t : group * t + group, :] for t in range(count)]
    span = range(group)

    def lane_of(x, k):
        return jnp.broadcast_to(x[:, k : k + 1], (group, size))

    def row_of(x, r):
        return jnp.broadcast_to(x[r : r + 1, :], (group, size))

    cols = [lane_of(rows[0], j) for j in span]
    for s in range(count):
        k = group * s
        more = s + 1 < count
        window = (lane >= k) & (lane < k + group)
        c = [[lane_of(rows[t], k + i) for i in span] for t in range(s + 1, count)]
        if more:
            ahead = [lane_of(rows[s + 1], k + group + j) for j in span]
            x = list(c[0])
        pivot = [[row_of(cols[j], i) if j >= i else None for j in span] for i in span]
        base = jnp.where(window, jnp.where(lane - k == sub, 1.0, 0.0), rows[s])
        u = [row_of(base, i) for i in span]
        scale = [None] * group
        for i in span:
            scale[i] = lax.rsqrt(pivot[i][i])
            u[i] = u[i] * scale[i]
            for j in range(i + 1, group):
                pivot[i][j] = pivot[i][j] * scale[i]
            if more:
                x[i] = x[i] * scale[i]
            for j in range(i + 1, group):
                u[j] = u[j] - pivot[i][j] * u[i]
                if more:
                    x[j] = x[j] - pivot[i][j] * x[i]
                for m in range(j, group):
                    pivot[j][m] = pivot[j][m] - pivot[i][j] * pivot[i][m]
            if more:
                for j in span:
                    ahead[j] = ahead[j] - x[i] * row_of(x[i], j)
        out = u[0]
        for i in range(1, group):
            out = jnp.where(sub == i, u[i], out)
        rows[s] = jnp.where(lane - k <= sub, out, 0.0)
        w = list(u)
        for i in reversed(span):
            w[i] = w[i] * scale[i]
            for j in range(i):
                w[j] = w[j] - pivot[j][i] * w[i]
        for t in range(s + 1, count):
            new = jnp.where(window, 0.0, rows[t])
            for i in reversed(span):
                new = new - c[t - s - 1][i] * w[i]
            rows[t] = new
        if more:
            cols = ahead
    return jnp.concatenate(rows, 0)


def kernel(
    ny, s_ref, c_ref, d_ref, f_ref, o_ref,
    gathered, low, work, inverse, solved, others,
    s_recv, s_send_z, s_send_y, c_recv, c_send, y_recv, y_send_z, y_send_y,
):
    extra, total = s_ref.shape
    count = total // T
    per = T // extra
    n = total // extra
    nz = n // ny
    me = lax.axis_index("blk")
    z, y = me // ny, me % ny
    link, links = lax.axis_index("chain"), lax.axis_size("chain")
    mine = pl.ds(pl.multiple_of(me * extra, extra), extra)
    tail = pl.ds(total, extra)
    z_peers = [(lax.rem(z + i, nz) * ny + y) for i in range(1, nz)]
    y_peers = [(z * ny + lax.rem(y + i, ny)) for i in range(1, ny)]
    has_next, has_prior = link + 1 < links, link > 0

    def tile(i):
        return pl.ds(pl.multiple_of(i * T, T), T)

    def rows_of(b):
        return pl.ds(pl.multiple_of(b * extra, extra), extra)

    def remote(src, dst, send, recv, **to):
        return pltpu.make_async_remote_copy(
            src_ref=src, dst_ref=dst, send_sem=send, recv_sem=recv, device_id=to, device_id_type=MESH
        )

    barrier = pltpu.get_barrier_semaphore()
    for peer in z_peers + y_peers:
        pl.semaphore_signal(barrier, inc=1, device_id={"blk": peer}, device_id_type=MESH)
    for has, step in ((has_next, 1), (has_prior, -1)):

        @pl.when(has)
        def _():
            pl.semaphore_signal(barrier, inc=1, device_id={"chain": link + step}, device_id_type=MESH)

    pl.semaphore_wait(barrier, nz + ny - 2 + has_next.astype(jnp.int32) + has_prior.astype(jnp.int32))

    def s_own(k):
        src = s_ref.at[:, tile(k)]
        dst = gathered.at[k, mine, :]
        out = []
        for i, peer in enumerate(z_peers):
            out.append(remote(src, dst, s_send_z.at[k, i], s_recv.at[k, me], blk=peer))
        for i, peer in enumerate(y_peers):
            out.append(remote(src, dst, s_send_y.at[k, z, i], s_recv.at[k, me], blk=peer))
        return out

    def s_from(k, b):
        at = gathered.at[k, rows_of(b), :]
        return remote(at, at, s_send_z.at[k, 0], s_recv.at[k, b], blk=z_peers[0])

    def s_on(k, zz):
        at = gathered.at[k, rows_of(zz * ny + y), :]
        return [
            remote(at, at, s_send_y.at[k, zz, i], s_recv.at[k, zz * ny + y], blk=peer)
            for i, peer in enumerate(y_peers)
        ]

    def s_has(k, b):
        return (b * extra) // T >= k

    def s_forward(k, zz):
        @pl.when((zz != z) & s_has(k, zz * ny + y))
        def _():
            s_from(k, zz * ny + y).wait_recv()
            for copy in s_on(k, zz):
                copy.start()

    def s_wait(k, i):
        for q in range(per):
            b = i * per + q

            @pl.when(b % ny != y)
            def _():
                s_from(k, b).wait_recv()

    def over_z(first, visit):
        def step(zz, _):
            visit(zz)
            return 0

        lax.fori_loop(first, nz, step, 0)

    def over(first, last, visit):
        def step(k, _):
            visit(k)
            return 0

        lax.fori_loop(first, last, step, 0)

    def start_own(k):
        @pl.when(s_has(k, me))
        def _():
            for copy in s_own(k):
                copy.start()

    over(0, count, start_own)

    def y_hop(k):
        at = others.at[k, mine, :]
        return remote(solved.at[k], at, c_send.at[k], c_recv.at[k], chain=lax.min(link + 1, links - 1))

    def y_own(k):
        at = others.at[k, mine, :]
        out = []
        for i, peer in enumerate(z_peers):
            out.append(remote(at, at, y_send_z.at[k, i], y_recv.at[k, me], blk=peer))
        for i, peer in enumerate(y_peers):
            out.append(remote(at, at, y_send_y.at[k, z, i], y_recv.at[k, me], blk=peer))
        return out

    def y_from(k, b):
        at = others.at[k, rows_of(b), :]
        return remote(at, at, y_send_z.at[k, 0], y_recv.at[k, b], blk=z_peers[0])

    def y_on(k, zz):
        at = others.at[k, rows_of(zz * ny + y), :]
        return [
            remote(at, at, y_send_y.at[k, zz, i], y_recv.at[k, zz * ny + y], blk=peer)
            for i, peer in enumerate(y_peers)
        ]

    def y_spread(k):
        y_hop(k).wait_recv()
        for copy in y_own(k):
            copy.start()

    def y_forward(k):
        def visit(zz):
            @pl.when(zz != z)
            def _():
                y_from(k, zz * ny + y).wait_recv()
                for copy in y_on(k, zz):
                    copy.start()

        over_z(0, visit)

    def y_use(k):
        def arrive(b):
            @pl.when(b % ny != y)
            def _():
                y_from(k, b).wait_recv()

        over(0, n, arrive)
        own = others[k, mine, :]

        def visit(j):
            o_ref[:, tile(j)] = o_ref[:, tile(j)] - dot_t(own, others[k, tile(j), :])

        over(0, count, visit)

    def y_stage(k):
        for lag, act in ((1, y_spread), (2, y_forward), (3, y_use)):

            @pl.when(has_prior & (k >= lag) & (k - lag < count))
            def _():
                act(k - lag)

    def keep(k):
        gathered[k, mine, :] = s_ref[:, tile(k)]
        o_ref[:, tile(k)] = d_ref[:, tile(k)]

    over(0, count, keep)
    s_forward(0, 0)

    def bring(k, rr, value):
        work[rr, :] = value.astype(F32)

        def step(j):
            work[rr, :] = work[rr, :] - product_t(low[j, rr, :], low[j, tile(k), :])

        over(0, k, step)

    def solve(k, rr):
        x = product_t(pair(work[rr, :]), inverse[...])
        low[k, rr, :] = pair(x)
        return x

    def chunk(k):
        s_wait(k, k)
        bring(k, tile(k), gathered[k, tile(k), :])
        at = pl.multiple_of(k * T, T)
        first, second = pl.ds(at, B), pl.ds(pl.multiple_of(at + B, B), B)
        n1 = invert(work[first, :B])
        x21 = product_t(pair(work[second, :B]), pair(n1))
        p21 = pair(x21)
        n2 = invert(work[second, B:] - product_t(p21, p21))
        m21 = product(n2, product(x21, n1))
        inverse[:B, :] = pair(jnp.concatenate([n1, jnp.zeros((B, B), F32)], 1))
        inverse[B:, :] = pair(jnp.concatenate([-m21, n2], 1))

        @pl.when(k == 0)
        def _():
            over_z(1, lambda zz: s_forward(0, zz))

        bring(k, tail, c_ref[:, tile(k)])
        solved[k] = solve(k, tail).astype(BF)
        solve(k, tile(k))

        def rest(i):
            s_wait(k, i)
            bring(k, tile(i), gathered[k, tile(i), :])
            solve(k, tile(i))

        over(k + 1, count, rest)

        @pl.when(has_next)
        def _():
            y_hop(k).start()

        row = me * extra + lax.broadcasted_iota(jnp.int32, (extra, T), 0)
        column = k * T + lax.broadcasted_iota(jnp.int32, (extra, T), 1)

        @pl.when(s_has(k, me))
        def _():
            both = low[k, mine, :]
            f_ref[:, tile(k)] = jnp.where(row >= column, both[:, :T].astype(F32) + both[:, T:].astype(F32), 0.0)

        @pl.when(jnp.logical_not(s_has(k, me)))
        def _():
            f_ref[:, tile(k)] = jnp.zeros((extra, T), F32)

        @pl.when(k + 1 < count)
        def _():
            over_z(0, lambda zz: s_forward(k + 1, zz))

        y_stage(k)

    over(0, count, chunk)
    over(count, count + 3, y_stage)

    def settle(k):
        @pl.when(s_has(k, me))
        def _():
            for copy in s_own(k):
                copy.wait_send()

        def visit(zz):
            @pl.when((zz != z) & s_has(k, zz * ny + y))
            def _():
                for copy in s_on(k, zz):
                    copy.wait_send()

            @pl.when((zz != z) & has_prior)
            def _():
                for copy in y_on(k, zz):
                    copy.wait_send()

        over_z(0, visit)

        @pl.when(has_prior)
        def _():
            for copy in y_own(k):
                copy.wait_send()

        @pl.when(has_next)
        def _():
            y_hop(k).wait_send()

    over(0, count, settle)


def local(schur, coupling, next_diag):
    extra, total = schur.shape
    n = lax.axis_size("blk")
    ny = 1 << ((n.bit_length() - 1) // 2)
    nz = n // ny
    count = total // T
    vmem = pl.BlockSpec(memory_space=pltpu.VMEM)
    sems = pltpu.SemaphoreType.DMA
    return pl.pallas_call(
        functools.partial(kernel, ny),
        out_shape=(jax.ShapeDtypeStruct((extra, total), F32),) * 2,
        in_specs=[vmem] * 3,
        out_specs=(vmem, vmem),
        scratch_shapes=[
            pltpu.VMEM((count, total, T), BF),
            pltpu.VMEM((count, total + extra, 2 * T), BF),
            pltpu.VMEM((total + extra, T), F32),
            pltpu.VMEM((T, 2 * T), BF),
            pltpu.VMEM((count, extra, T), BF),
            pltpu.VMEM((count, total, T), BF),
            sems((count, n)),
            sems((count, nz - 1)),
            sems((count, nz, max(ny - 1, 1))),
            sems((count,)),
            sems((count,)),
            sems((count, n)),
            sems((count, nz - 1)),
            sems((count, nz, max(ny - 1, 1))),
        ],
        compiler_params=pltpu.CompilerParams(
            vmem_limit_bytes=60 * 1024 * 1024, collective_id=0, has_side_effects=True
        ),
        name="slab_step",
    )(schur, coupling, next_diag)


def solution(mesh):
    placed = (P(("chain", "blk"), None),) * 3
    return jax.shard_map(
        local, mesh=mesh, in_specs=placed, out_specs=(P(("chain", "blk"), None),) * 2, check_vma=False
    )
```

```python
import functools
import jax
import jax.numpy as jnp
from jax import lax
from jax.experimental import pallas as pl
from jax.experimental.pallas import tpu as pltpu
from jax.sharding import PartitionSpec as P

B = 128
T = 2 * B
LAG = 2
USE = 2
BF = jnp.bfloat16
F32 = jnp.float32
MESH = pl.DeviceIdType.MESH


def split(x):
    hi = x.astype(BF)
    return hi, (x - hi.astype(F32)).astype(BF)


def dot_t(a, b):
    return lax.dot_general(a, b, (((1,), (1,)), ((), ())), preferred_element_type=F32)


def pair(x):
    return jnp.concatenate(split(x), 1)


def product_t(a, b):
    half = a.shape[1] // 2
    return dot_t(jnp.concatenate([a[:, :half], a], 1), jnp.concatenate([b, b[:, :half]], 1))


def product(a, b):
    ah, al = split(a)
    bh, bl = split(b)
    return jnp.dot(
        jnp.concatenate([ah, ah, al], 1), jnp.concatenate([bh, bl, bh], 0), preferred_element_type=F32
    )


def invert(block, beside=()):
    size = block.shape[0]
    group = 8
    count = size // group
    sub = lax.broadcasted_iota(jnp.int32, (group, size), 0)
    lane = lax.broadcasted_iota(jnp.int32, (group, size), 1)
    rows = [block[group * t : group * t + group, :] for t in range(count)]
    span = range(group)

    def lane_of(x, k):
        return jnp.broadcast_to(x[:, k : k + 1], (group, size))

    def row_of(x, r):
        return jnp.broadcast_to(x[r : r + 1, :], (group, size))

    cols = [lane_of(rows[0], j) for j in span]
    for s in range(count):
        k = group * s
        more = s + 1 < count
        window = (lane >= k) & (lane < k + group)
        c = [[lane_of(rows[t], k + i) for i in span] for t in range(s + 1, count)]
        if more:
            ahead = [lane_of(rows[s + 1], k + group + j) for j in span]
            x = list(c[0])
        pivot = [[row_of(cols[j], i) if j >= i else None for j in span] for i in span]
        base = jnp.where(window, jnp.where(lane - k == sub, 1.0, 0.0), rows[s])
        u = [row_of(base, i) for i in span]
        scale = [None] * group
        for i in span:
            scale[i] = lax.rsqrt(pivot[i][i])
            u[i] = u[i] * scale[i]
            for j in range(i + 1, group):
                pivot[i][j] = pivot[i][j] * scale[i]
            if more:
                x[i] = x[i] * scale[i]
            for j in range(i + 1, group):
                u[j] = u[j] - pivot[i][j] * u[i]
                if more:
                    x[j] = x[j] - pivot[i][j] * x[i]
                for m in range(j, group):
                    pivot[j][m] = pivot[j][m] - pivot[i][j] * pivot[i][m]
            if more:
                for j in span:
                    ahead[j] = ahead[j] - x[i] * row_of(x[i], j)
        out = u[0]
        for i in range(1, group):
            out = jnp.where(sub == i, u[i], out)
        rows[s] = jnp.where(lane - k <= sub, out, 0.0)
        w = list(u)
        for i in reversed(span):
            w[i] = w[i] * scale[i]
            for j in range(i):
                w[j] = w[j] - pivot[j][i] * w[i]
        for t in range(s + 1, count):
            new = jnp.where(window, 0.0, rows[t])
            for i in reversed(span):
                new = new - c[t - s - 1][i] * w[i]
            rows[t] = new
        if s % 2 and s // 2 < len(beside):
            beside[s // 2]()
        if more:
            cols = ahead
    return jnp.concatenate(rows, 0)


def kernel(
    ny, s_ref, c_ref, d_ref, f_ref, o_ref,
    gathered, low, work, inverse, solved, others,
    s_recv, s_send_z, s_send_y, c_recv, c_send, y_recv, y_send_z, y_send_y, s_direct, y_direct,
):
    extra, total = s_ref.shape
    count = total // T
    per = T // extra
    n = total // extra
    nz = n // ny
    me = lax.axis_index("blk")
    z, y = me // ny, me % ny
    link, links = lax.axis_index("chain"), lax.axis_size("chain")
    mine = pl.ds(pl.multiple_of(me * extra, extra), extra)
    tail = pl.ds(total, extra)
    up, down = lax.min(z + 1, nz - 1) * ny + y, lax.max(z - 1, 0) * ny + y
    has_up, has_down = z + 1 < nz, z > 0
    z_peers = [lax.rem(z + i, nz) * ny + y for i in range(1, nz)]
    y_peers = [(z * ny + lax.rem(y + i, ny)) for i in range(1, ny)]
    has_next, has_prior = link + 1 < links, link > 0

    def tile(i):
        return pl.ds(pl.multiple_of(i * T, T), T)

    def rows_of(b):
        return pl.ds(pl.multiple_of(b * extra, extra), extra)

    def remote(src, dst, send, recv, **to):
        return pltpu.make_async_remote_copy(
            src_ref=src, dst_ref=dst, send_sem=send, recv_sem=recv, device_id=to, device_id_type=MESH
        )

    barrier = pltpu.get_barrier_semaphore()
    greeted = jnp.int32(nz + ny - 2)
    for peer in z_peers + y_peers:
        pl.semaphore_signal(barrier, inc=1, device_id={"blk": peer}, device_id_type=MESH)
    for has, to in (
        (has_next, {"chain": link + 1}),
        (has_prior, {"chain": link - 1}),
    ):
        greeted = greeted + has.astype(jnp.int32)

        @pl.when(has)
        def _():
            pl.semaphore_signal(barrier, inc=1, device_id=to, device_id_type=MESH)

    pl.semaphore_wait(barrier, greeted)

    def along_z(zz):
        return ((zz <= z) & has_up, up, 0), ((zz >= z) & has_down, down, 1)

    def passing(src, dst, k, zz, send_z, send_y, recv, act, straight, direct):
        at = recv.at[k, zz * ny + y]

        @pl.when(straight & (zz == z))
        def _():
            for i, peer in enumerate(z_peers):
                act(remote(src, dst, direct.at[lax.rem(k, 2), i], at, blk=peer))

        for has, peer, way in along_z(zz):

            @pl.when(has & jnp.logical_not(straight))
            def _():
                act(remote(src, dst, send_z.at[k, zz, way], at, blk=peer))

        for i, peer in enumerate(y_peers):
            act(remote(src, dst, send_y.at[k, zz, i], at, blk=peer))

    def begin(copy):
        copy.start()

    def end(copy):
        copy.wait_send()

    def s_pass(k, zz, act):
        at = gathered.at[k, rows_of(zz * ny + y), :]
        passing(at, at, k, zz, s_send_z, s_send_y, s_recv, act, k < 2, s_direct)

    def s_own(k, act):
        dst = gathered.at[k, mine, :]
        passing(s_ref.at[:, tile(k)], dst, k, z, s_send_z, s_send_y, s_recv, act, k < 2, s_direct)

    def s_from(k, b):
        at = gathered.at[k, rows_of(b), :]
        return remote(at, at, s_send_z.at[k, 0, 0], s_recv.at[k, b], blk=up)

    def s_has(k, b):
        return (b * extra) // T >= k

    def both_ways(d, visit):
        for zz in (z - d, z + d):

            @pl.when((zz >= 0) & (zz < nz))
            def _():
                visit(zz)

    def first(k, b):
        return (k == 0) & (b < per)

    def s_forward(k, d):
        def visit(zz):
            @pl.when(s_has(k, zz * ny + y) & jnp.logical_not(first(k, zz * ny + y)))
            def _():
                s_from(k, zz * ny + y).wait_recv()
                s_pass(k, zz, begin)

        both_ways(d, visit)

    def s_wait(k, i):
        for q in range(per):
            b = i * per + q

            @pl.when(b % ny != y)
            def _():
                s_from(k, b).wait_recv()

    def over(first, last, visit):
        def step(k, _):
            visit(k)
            return 0

        lax.fori_loop(first, last, step, 0)

    def start_own(k):
        @pl.when((k < count) & s_has(k, me))
        def _():
            s_own(k, begin)

    for k in range(3):
        start_own(k)

    def y_hop(k):
        at = others.at[k, mine, :]
        return remote(solved.at[k], at, c_send.at[k], c_recv.at[k], chain=lax.min(link + 1, links - 1))

    def y_pass(k, zz, act):
        at = others.at[k, rows_of(zz * ny + y), :]
        passing(at, at, k, zz, y_send_z, y_send_y, y_recv, act, k == count - 1, y_direct)

    def y_from(k, b):
        at = others.at[k, rows_of(b), :]
        return remote(at, at, y_send_z.at[k, 0, 0], y_recv.at[k, b], blk=up)

    def y_spread(k):
        y_hop(k).wait_recv()
        y_pass(k, z, begin)

    def y_forward(k, d):
        def visit(zz):
            y_from(k, zz * ny + y).wait_recv()
            y_pass(k, zz, begin)

        both_ways(d, visit)

    def y_use(k):
        def arrive(b):
            @pl.when(b % ny != y)
            def _():
                y_from(k, b).wait_recv()

        over(0, n, arrive)
        own = others[k, mine, :]

        def visit(j):
            o_ref[:, tile(j)] = o_ref[:, tile(j)] - dot_t(own, others[k, tile(j), :])

        over(0, count, visit)

    def when_y(k, act):
        @pl.when(has_prior & (k >= 0) & (k < count))
        def _():
            act(k)

    reach = ([1], [2], list(range(3, nz)))

    def s_tick(k, ds):
        @pl.when(k < count)
        def _():
            for d in ds:
                s_forward(k, d)

    steps = [(min(d, 3) * LAG, d) for d in range(1, nz)]
    last = 3 * LAG + USE

    def y_tick(k, p):
        def due(lag):
            return (p - 2 - lag) % 3 == 0, k + (p - 2 - lag) // 3

        for lag, d in steps:
            now, m = due(lag)
            if now:
                when_y(m, lambda m: y_forward(m, d))
        now, m = due(last)
        if now:
            when_y(m, y_use)
        if p == 2:
            when_y(k, y_spread)

    def tick(k, p):
        if p < 2:

            @pl.when(k == 0)
            def _():
                s_tick(p, range(1, nz))

        s_tick(k + 2, reach[p])
        if p == 1:
            start_own(k + 3)
        y_tick(k, p)

    def keep(k):
        gathered[k, mine, :] = s_ref[:, tile(k)]
        o_ref[:, tile(k)] = d_ref[:, tile(k)]

    over(0, count, keep)
    for b in range(per):

        @pl.when((b % ny == y) & (b // ny != z))
        def _():
            s_from(0, b).wait_recv()
            s_pass(0, b // ny, begin)


    even = extra == T
    slots = max((count - k) * k for k in range(count)) if even else 0

    def minus(k, j, rr):
        return product_t(low[j, rr, :], low[j, tile(k), :])

    def bring(k, rr, value):
        work[rr, :] = value.astype(F32)

        def step(j):
            work[rr, :] = work[rr, :] - minus(k, j, rr)

        over(0, k, step)

    def beside(k, q):
        every = lax.max(k, 1)
        i, j = lax.min(k + 1 + q // every, count), lax.rem(q, every)
        to = tile(jnp.where(q < (count - k) * k, i, count + 1))
        held = jnp.where(j == 0, 0.0, work[to, :])
        work[to, :] = held - minus(k, j, tile(i))

    def settle_rows(k, rr, value):
        if even:
            work[rr, :] = jnp.where(k == 0, 0.0, work[rr, :]) + value.astype(F32)
        else:
            bring(k, rr, value)

    def solve(k, rr):
        x = product_t(pair(work[rr, :]), inverse[...])
        low[k, rr, :] = pair(x)
        return x

    def chunk(k):
        s_wait(k, k)
        bring(k, tile(k), gathered[k, tile(k), :])
        at = pl.multiple_of(k * T, T)
        first, second = pl.ds(at, B), pl.ds(pl.multiple_of(at + B, B), B)
        later = [functools.partial(beside, k, jnp.int32(q)) for q in range(slots)]
        n1 = invert(work[first, :B], later[: slots // 2])
        tick(k, 0)
        x21 = product_t(pair(work[second, :B]), pair(n1))
        p21 = pair(x21)
        n2 = invert(work[second, B:] - product_t(p21, p21), later[slots // 2 :])
        m21 = product(n2, product(x21, n1))
        inverse[:B, :] = pair(jnp.concatenate([n1, jnp.zeros((B, B), F32)], 1))
        inverse[B:, :] = pair(jnp.concatenate([-m21, n2], 1))

        tick(k, 1)
        settle_rows(k, tail, c_ref[:, tile(k)])
        solved[k] = solve(k, tail).astype(BF)

        solve(k, tile(k))

        @pl.when(has_next)
        def _():
            y_hop(k).start()

        def rest(i):
            s_wait(k, i)
            settle_rows(k, tile(i), gathered[k, tile(i), :])
            solve(k, tile(i))

        over(k + 1, count, rest)

        row = me * extra + lax.broadcasted_iota(jnp.int32, (extra, T), 0)
        column = k * T + lax.broadcasted_iota(jnp.int32, (extra, T), 1)

        @pl.when(s_has(k, me))
        def _():
            both = low[k, mine, :]
            f_ref[:, tile(k)] = jnp.where(row >= column, both[:, :T].astype(F32) + both[:, T:].astype(F32), 0.0)

        @pl.when(jnp.logical_not(s_has(k, me)))
        def _():
            f_ref[:, tile(k)] = jnp.zeros((extra, T), F32)

        tick(k, 2)

    over(0, count, chunk)

    def drain(k):
        for p in range(3):
            y_tick(k, p)

    over(count, count + (last + 4) // 3, drain)

    def settle(k):
        @pl.when(s_has(k, me))
        def _():
            s_own(k, end)

        @pl.when(has_prior)
        def _():
            y_pass(k, z, end)

        def visit(zz):
            @pl.when((zz != z) & s_has(k, zz * ny + y))
            def _():
                s_pass(k, zz, end)

            @pl.when((zz != z) & has_prior)
            def _():
                y_pass(k, zz, end)

        over(0, nz, visit)

        @pl.when(has_next)
        def _():
            y_hop(k).wait_send()

    over(0, count, settle)


def local(schur, coupling, next_diag):
    extra, total = schur.shape
    n = lax.axis_size("blk")
    ny = 1 << ((n.bit_length() - 1) // 2)
    nz = n // ny
    count = total // T
    vmem = pl.BlockSpec(memory_space=pltpu.VMEM)
    sems = pltpu.SemaphoreType.DMA
    return pl.pallas_call(
        functools.partial(kernel, ny),
        out_shape=(jax.ShapeDtypeStruct((extra, total), F32),) * 2,
        in_specs=[vmem] * 3,
        out_specs=(vmem, vmem),
        scratch_shapes=[
            pltpu.VMEM((count, total, T), BF),
            pltpu.VMEM((count, total + extra, 2 * T), BF),
            pltpu.VMEM((total + extra + T, T), F32),
            pltpu.VMEM((T, 2 * T), BF),
            pltpu.VMEM((count, extra, T), BF),
            pltpu.VMEM((count, total, T), BF),
            sems((count, n)),
            sems((count, nz, 2)),
            sems((count, nz, max(ny - 1, 1))),
            sems((count,)),
            sems((count,)),
            sems((count, n)),
            sems((count, nz, 2)),
            sems((count, nz, max(ny - 1, 1))),
            sems((2, nz - 1)),
            sems((2, nz - 1)),
        ],
        compiler_params=pltpu.CompilerParams(
            vmem_limit_bytes=60 * 1024 * 1024, collective_id=0, has_side_effects=True
        ),
        name="slab_step",
    )(schur, coupling, next_diag)


def solution(mesh):
    placed = (P(("chain", "blk"), None),) * 3
    return jax.shard_map(
        local, mesh=mesh, in_specs=placed, out_specs=(P(("chain", "blk"), None),) * 2, check_vma=False
    )
```

```python
import functools
import jax
import jax.numpy as jnp
from jax import lax
from jax.experimental import pallas as pl
from jax.experimental.pallas import tpu as pltpu
from jax.sharding import PartitionSpec as P

B = 128
T = 2 * B
LAG = 2
USE = 4
BF = jnp.bfloat16
F32 = jnp.float32
MESH = pl.DeviceIdType.MESH


def split(x):
    hi = x.astype(BF)
    return hi, (x - hi.astype(F32)).astype(BF)


def dot_t(a, b):
    return lax.dot_general(a, b, (((1,), (1,)), ((), ())), preferred_element_type=F32)


def pair(x):
    return jnp.concatenate(split(x), 1)


def product_t(a, b):
    half = a.shape[1] // 2
    return dot_t(jnp.concatenate([a[:, :half], a], 1), jnp.concatenate([b, b[:, :half]], 1))


def product(a, b):
    ah, al = split(a)
    bh, bl = split(b)
    return jnp.dot(
        jnp.concatenate([ah, ah, al], 1), jnp.concatenate([bh, bl, bh], 0), preferred_element_type=F32
    )


def invert(block, beside=()):
    size = block.shape[0]
    group = 8
    count = size // group
    sub = lax.broadcasted_iota(jnp.int32, (group, size), 0)
    lane = lax.broadcasted_iota(jnp.int32, (group, size), 1)
    rows = [block[group * t : group * t + group, :] for t in range(count)]
    span = range(group)

    def lane_of(x, k):
        return jnp.broadcast_to(x[:, k : k + 1], (group, size))

    def row_of(x, r):
        return jnp.broadcast_to(x[r : r + 1, :], (group, size))

    cols = [lane_of(rows[0], j) for j in span]
    for s in range(count):
        k = group * s
        more = s + 1 < count
        window = (lane >= k) & (lane < k + group)
        c = [[lane_of(rows[t], k + i) for i in span] for t in range(s + 1, count)]
        if more:
            ahead = [lane_of(rows[s + 1], k + group + j) for j in span]
            x = list(c[0])
        pivot = [[row_of(cols[j], i) if j >= i else None for j in span] for i in span]
        base = jnp.where(window, jnp.where(lane - k == sub, 1.0, 0.0), rows[s])
        u = [row_of(base, i) for i in span]
        scale = [None] * group
        for i in span:
            scale[i] = lax.rsqrt(pivot[i][i])
            u[i] = u[i] * scale[i]
            for j in range(i + 1, group):
                pivot[i][j] = pivot[i][j] * scale[i]
            if more:
                x[i] = x[i] * scale[i]
            for j in range(i + 1, group):
                u[j] = u[j] - pivot[i][j] * u[i]
                if more:
                    x[j] = x[j] - pivot[i][j] * x[i]
                for m in range(j, group):
                    pivot[j][m] = pivot[j][m] - pivot[i][j] * pivot[i][m]
            if more:
                for j in span:
                    ahead[j] = ahead[j] - x[i] * row_of(x[i], j)
        out = u[0]
        for i in range(1, group):
            out = jnp.where(sub == i, u[i], out)
        rows[s] = jnp.where(lane - k <= sub, out, 0.0)
        w = list(u)
        for i in reversed(span):
            w[i] = w[i] * scale[i]
            for j in range(i):
                w[j] = w[j] - pivot[j][i] * w[i]
        for t in range(s + 1, count):
            new = jnp.where(window, 0.0, rows[t])
            for i in reversed(span):
                new = new - c[t - s - 1][i] * w[i]
            rows[t] = new
        if s % 2 and s // 2 < len(beside):
            beside[s // 2]()
        if more:
            cols = ahead
    return jnp.concatenate(rows, 0)


def kernel(
    ny, s_ref, c_ref, d_ref, f_ref, o_ref,
    gathered, low, work, inverse, solved, others, lent, part, part_in,
    s_recv, s_send_z, s_send_y, c_recv, c_send, y_recv, y_send_z, y_send_y, s_direct, y_direct, l_recv, l_send_z, l_send_y, p_sem,
):
    extra, total = s_ref.shape
    count = total // T
    per = T // extra
    n = total // extra
    nz = n // ny
    me = lax.axis_index("blk")
    z, y = me // ny, me % ny
    link, links = lax.axis_index("chain"), lax.axis_size("chain")
    mine = pl.ds(pl.multiple_of(me * extra, extra), extra)
    tail = pl.ds(total, extra)
    up, down = lax.min(z + 1, nz - 1) * ny + y, lax.max(z - 1, 0) * ny + y
    has_up, has_down = z + 1 < nz, z > 0
    z_peers = [lax.rem(z + i, nz) * ny + y for i in range(1, nz)]
    y_peers = [(z * ny + lax.rem(y + i, ny)) for i in range(1, ny)]
    has_next, has_prior = link + 1 < links, link > 0
    shared = 3 * count // 8
    lends = has_next & (link % 2 == 1)
    borrows = has_prior & (link % 2 == 0)

    def hops(k):
        return has_next & ((link % 2 == 0) | (k >= shared))

    def comes(k):
        return has_prior & ((link % 2 == 1) | (k >= shared))


    def tile(i):
        return pl.ds(pl.multiple_of(i * T, T), T)

    def rows_of(b):
        return pl.ds(pl.multiple_of(b * extra, extra), extra)

    def remote(src, dst, send, recv, **to):
        return pltpu.make_async_remote_copy(
            src_ref=src, dst_ref=dst, send_sem=send, recv_sem=recv, device_id=to, device_id_type=MESH
        )

    barrier = pltpu.get_barrier_semaphore()
    greeted = jnp.int32(nz + ny - 2)
    for peer in z_peers + y_peers:
        pl.semaphore_signal(barrier, inc=1, device_id={"blk": peer}, device_id_type=MESH)
    for has, to in (
        (has_next, {"chain": link + 1}),
        (has_prior, {"chain": link - 1}),
    ):
        greeted = greeted + has.astype(jnp.int32)

        @pl.when(has)
        def _():
            pl.semaphore_signal(barrier, inc=1, device_id=to, device_id_type=MESH)

    pl.semaphore_wait(barrier, greeted)

    def along_z(zz):
        return ((zz <= z) & has_up, up, 0), ((zz >= z) & has_down, down, 1)

    def passing(src, dst, k, zz, send_z, send_y, recv, act, straight, direct):
        at = recv.at[k, zz * ny + y]

        @pl.when(straight & (zz == z))
        def _():
            for i, peer in enumerate(z_peers):
                act(remote(src, dst, direct.at[lax.rem(k, 2), i], at, blk=peer))

        for has, peer, way in along_z(zz):

            @pl.when(has & jnp.logical_not(straight))
            def _():
                act(remote(src, dst, send_z.at[k, zz, way], at, blk=peer))

        for i, peer in enumerate(y_peers):
            act(remote(src, dst, send_y.at[k, zz, i], at, blk=peer))

    def begin(copy):
        copy.start()

    def end(copy):
        copy.wait_send()

    def s_pass(k, zz, act):
        at = gathered.at[k, rows_of(zz * ny + y), :]
        passing(at, at, k, zz, s_send_z, s_send_y, s_recv, act, k < 2, s_direct)

    def s_own(k, act):
        dst = gathered.at[k, mine, :]
        passing(s_ref.at[:, tile(k)], dst, k, z, s_send_z, s_send_y, s_recv, act, k < 2, s_direct)

    def s_from(k, b):
        at = gathered.at[k, rows_of(b), :]
        return remote(at, at, s_send_z.at[k, 0, 0], s_recv.at[k, b], blk=up)

    def s_has(k, b):
        return (b * extra) // T >= k

    def both_ways(d, visit):
        for zz in (z - d, z + d):

            @pl.when((zz >= 0) & (zz < nz))
            def _():
                visit(zz)

    def first(k, b):
        return (k == 0) & (b < per)

    def s_forward(k, d):
        def visit(zz):
            @pl.when(s_has(k, zz * ny + y) & jnp.logical_not(first(k, zz * ny + y)))
            def _():
                s_from(k, zz * ny + y).wait_recv()
                s_pass(k, zz, begin)

        both_ways(d, visit)

    def s_wait(k, i):
        for q in range(per):
            b = i * per + q

            @pl.when(b % ny != y)
            def _():
                s_from(k, b).wait_recv()

    def over(first, last, visit):
        def step(k, _):
            visit(k)
            return 0

        lax.fori_loop(first, last, step, 0)

    def start_own(k):
        @pl.when((k < count) & s_has(k, me))
        def _():
            s_own(k, begin)

    for k in range(3):
        start_own(k)

    def y_hop(k):
        at = others.at[k, mine, :]
        return remote(solved.at[k], at, c_send.at[k], c_recv.at[k], chain=lax.min(link + 1, links - 1))

    def y_pass(k, zz, act):
        at = others.at[k, rows_of(zz * ny + y), :]
        passing(at, at, k, zz, y_send_z, y_send_y, y_recv, act, k == count - 1, y_direct)

    def y_from(k, b):
        at = others.at[k, rows_of(b), :]
        return remote(at, at, y_send_z.at[k, 0, 0], y_recv.at[k, b], blk=up)

    def y_spread(k):
        y_hop(k).wait_recv()
        y_pass(k, z, begin)

    def y_forward(k, d):
        def visit(zz):
            y_from(k, zz * ny + y).wait_recv()
            y_pass(k, zz, begin)

        both_ways(d, visit)

    def y_use(k):
        def arrive(b):
            @pl.when(b % ny != y)
            def _():
                y_from(k, b).wait_recv()

        over(0, n, arrive)
        own = others[k, mine, :]

        def visit(j):
            o_ref[:, tile(j)] = o_ref[:, tile(j)] - dot_t(own, others[k, tile(j), :])

        over(0, count, visit)

    def l_pass(k, zz, src, act):
        dst = lent.at[k, rows_of(zz * ny + y), :]
        passing(src, dst, k, zz, l_send_z, l_send_y, l_recv, act, k < 0, y_direct)

    def l_from(k, b):
        at = lent.at[k, rows_of(b), :]
        return remote(at, at, l_send_z.at[k, 0, 0], l_recv.at[k, b], blk=up)

    def l_spread(k):
        lent[k, mine, :] = solved[k]
        l_pass(k, z, solved.at[k], begin)

    def l_forward(k, d):
        def visit(zz):
            l_from(k, zz * ny + y).wait_recv()
            l_pass(k, zz, lent.at[k, rows_of(zz * ny + y), :], begin)

        both_ways(d, visit)

    def l_use(k):
        def arrive(b):
            @pl.when(b % ny != y)
            def _():
                l_from(k, b).wait_recv()

        over(0, n, arrive)
        own = lent[k, mine, :]

        def visit(j):
            part[:, tile(j)] = part[:, tile(j)] + dot_t(own, lent[k, tile(j), :])

        over(0, count, visit)

    def part_hop():
        to = lax.min(link + 1, links - 1)
        return remote(part, part_in, p_sem.at[0], p_sem.at[1], chain=to)

    def when_y(k, act):
        @pl.when((k >= 0) & (k < count) & comes(k))
        def _():
            act(k)

    def when_l(k, act):
        @pl.when(lends & (k >= 0) & (k < shared))
        def _():
            act(k)

    reach = ([1], [2], list(range(3, nz)))

    def s_tick(k, ds):
        @pl.when(k < count)
        def _():
            for d in ds:
                s_forward(k, d)

    steps = [(min(d, 3) * LAG, d) for d in range(1, nz)]
    last = 3 * LAG + USE

    def y_tick(k, p):
        def due(lag):
            return (p - 2 - lag) % 3 == 0, k + (p - 2 - lag) // 3

        for lag, d in steps:
            now, m = due(lag)
            if now:
                when_y(m, lambda m: y_forward(m, d))
                when_l(m, lambda m: l_forward(m, d))
        now, m = due(last)
        if now:
            when_y(m, y_use)
            when_l(m, l_use)
        if p == 2:
            when_y(k, y_spread)
            when_l(k, l_spread)

            @pl.when(lends & (k == shared + (last + 2) // 3))
            def _():
                part_hop().start()

    def tick(k, p):
        if p < 2:

            @pl.when(k == 0)
            def _():
                s_tick(p, range(1, nz))

        s_tick(k + 2, reach[p])
        if p == 1:
            start_own(k + 3)
        y_tick(k, p)

    def keep(k):
        gathered[k, mine, :] = s_ref[:, tile(k)]
        o_ref[:, tile(k)] = d_ref[:, tile(k)]
        part[:, tile(k)] = jnp.zeros((extra, T), F32)

    over(0, count, keep)
    for b in range(per):

        @pl.when((b % ny == y) & (b // ny != z))
        def _():
            s_from(0, b).wait_recv()
            s_pass(0, b // ny, begin)


    even = extra == T
    slots = max((count - k) * k for k in range(count)) if even else 0

    def minus(k, j, rr):
        return product_t(low[j, rr, :], low[j, tile(k), :])

    def bring(k, rr, value):
        work[rr, :] = value.astype(F32)

        def step(j):
            work[rr, :] = work[rr, :] - minus(k, j, rr)

        over(0, k, step)

    def beside(k, q):
        every = lax.max(k, 1)
        i, j = lax.min(k + 1 + q // every, count), lax.rem(q, every)
        to = tile(jnp.where(q < (count - k) * k, i, count + 1))
        held = jnp.where(j == 0, 0.0, work[to, :])
        work[to, :] = held - minus(k, j, tile(i))

    def settle_rows(k, rr, value):
        if even:
            work[rr, :] = jnp.where(k == 0, 0.0, work[rr, :]) + value.astype(F32)
        else:
            bring(k, rr, value)

    def solve(k, rr):
        x = product_t(pair(work[rr, :]), inverse[...])
        low[k, rr, :] = pair(x)
        return x

    def chunk(k):
        s_wait(k, k)
        bring(k, tile(k), gathered[k, tile(k), :])
        at = pl.multiple_of(k * T, T)
        first, second = pl.ds(at, B), pl.ds(pl.multiple_of(at + B, B), B)
        later = [functools.partial(beside, k, jnp.int32(q)) for q in range(slots)]
        n1 = invert(work[first, :B], later[: slots // 2])
        tick(k, 0)
        x21 = product_t(pair(work[second, :B]), pair(n1))
        p21 = pair(x21)
        n2 = invert(work[second, B:] - product_t(p21, p21), later[slots // 2 :])
        m21 = product(n2, product(x21, n1))
        inverse[:B, :] = pair(jnp.concatenate([n1, jnp.zeros((B, B), F32)], 1))
        inverse[B:, :] = pair(jnp.concatenate([-m21, n2], 1))

        tick(k, 1)
        settle_rows(k, tail, c_ref[:, tile(k)])
        solved[k] = solve(k, tail).astype(BF)

        solve(k, tile(k))

        @pl.when(hops(k))
        def _():
            y_hop(k).start()

        def rest(i):
            s_wait(k, i)
            settle_rows(k, tile(i), gathered[k, tile(i), :])
            solve(k, tile(i))

        over(k + 1, count, rest)

        row = me * extra + lax.broadcasted_iota(jnp.int32, (extra, T), 0)
        column = k * T + lax.broadcasted_iota(jnp.int32, (extra, T), 1)

        @pl.when(s_has(k, me))
        def _():
            both = low[k, mine, :]
            f_ref[:, tile(k)] = jnp.where(row >= column, both[:, :T].astype(F32) + both[:, T:].astype(F32), 0.0)

        @pl.when(jnp.logical_not(s_has(k, me)))
        def _():
            f_ref[:, tile(k)] = jnp.zeros((extra, T), F32)

        tick(k, 2)

    over(0, count, chunk)

    def drain(k):
        for p in range(3):
            y_tick(k, p)

    over(count, count + (last + 4) // 3, drain)

    @pl.when(borrows)
    def _():
        part_hop().wait_recv()

        def fold(j):
            o_ref[:, tile(j)] = o_ref[:, tile(j)] - part_in[:, tile(j)]

        over(0, count, fold)

    @pl.when(lends)
    def _():
        part_hop().wait_send()

    def settle(k):
        @pl.when(s_has(k, me))
        def _():
            s_own(k, end)

        when_y(k, lambda m: y_pass(m, z, end))
        when_l(k, lambda m: l_pass(m, z, solved.at[m], end))

        def visit(zz):
            @pl.when((zz != z) & s_has(k, zz * ny + y))
            def _():
                s_pass(k, zz, end)

            @pl.when(zz != z)
            def _():
                when_y(k, lambda m: y_pass(m, zz, end))
                when_l(k, lambda m: l_pass(m, zz, lent.at[m, rows_of(zz * ny + y), :], end))

        over(0, nz, visit)

        @pl.when(hops(k))
        def _():
            y_hop(k).wait_send()

    over(0, count, settle)


def local(schur, coupling, next_diag):
    extra, total = schur.shape
    n = lax.axis_size("blk")
    ny = 1 << ((n.bit_length() - 1) // 2)
    nz = n // ny
    count = total // T
    vmem = pl.BlockSpec(memory_space=pltpu.VMEM)
    sems = pltpu.SemaphoreType.DMA
    return pl.pallas_call(
        functools.partial(kernel, ny),
        out_shape=(jax.ShapeDtypeStruct((extra, total), F32),) * 2,
        in_specs=[vmem] * 3,
        out_specs=(vmem, vmem),
        scratch_shapes=[
            pltpu.VMEM((count, total, T), BF),
            pltpu.VMEM((count, total + extra, 2 * T), BF),
            pltpu.VMEM((total + extra + T, T), F32),
            pltpu.VMEM((T, 2 * T), BF),
            pltpu.VMEM((count, extra, T), BF),
            pltpu.VMEM((count, total, T), BF),
            pltpu.VMEM((count // 2, total, T), BF),
            pltpu.VMEM((extra, total), F32),
            pltpu.VMEM((extra, total), F32),
            sems((count, n)),
            sems((count, nz, 2)),
            sems((count, nz, max(ny - 1, 1))),
            sems((count,)),
            sems((count,)),
            sems((count, n)),
            sems((count, nz, 2)),
            sems((count, nz, max(ny - 1, 1))),
            sems((2, nz - 1)),
            sems((2, nz - 1)),
            sems((count // 2, n)),
            sems((count // 2, nz, 2)),
            sems((count // 2, nz, max(ny - 1, 1))),
            sems((2,)),
        ],
        compiler_params=pltpu.CompilerParams(
            vmem_limit_bytes=60 * 1024 * 1024, collective_id=0, has_side_effects=True
        ),
        name="slab_step",
    )(schur, coupling, next_diag)


def solution(mesh):
    placed = (P(("chain", "blk"), None),) * 3
    return jax.shard_map(
        local, mesh=mesh, in_specs=placed, out_specs=(P(("chain", "blk"), None),) * 2, check_vma=False
    )
```
